256 devices in a mesh: rep: 16 (over y, z_hi, core), tp: 16 (over x, z_lo).
Axes of the slice: x: 4, y: 4, z: 8 (z_hi: 2, z_lo: 4; z = z_hi * 4 + z_lo), core: 2. Of those that a mesh axis runs over, the one named last changes fastest.
Arguments:
- activations: bfloat16 [16, 2048, 4096], P('rep', 'tp'), may hold values from -6 to 6
- cotangent: bfloat16 [16, 2048, 8192], P('rep', None, 'tp'), may hold values from -0.13183594 to 0.13183594
- drift: bfloat16 [16, 4096, 8192], P('rep', None, 'tp'), may hold values from -8 to 8
- outer_weights: float32 [4096, 8192], P(('rep', 'tp')), may hold values from -6 to 6
- momentum: float32 [4096, 8192], P(('rep', 'tp')), may hold values from -6 to 6
Outputs:
- weights: bfloat16 [4096, 8192], P(None, 'tp')
- new_outer: float32 [4096, 8192], P(('rep', 'tp'))
- new_momentum: float32 [4096, 8192], P(('rep', 'tp'))
The draws below stay inside these ranges and needn't reach their ends.
All inputs are finite; a program needn't handle non-finite values.
Results may differ from the reference program's by a relative error of at most 0.0085.
Values may be sent and summed in bfloat16 or wider, within the bound.
A program may use at most 128 MiB of HBM per device.

```python
import jax
import jax.numpy as jnp
from jax import lax

D = 4096
FFW = 8192
TOK = 2048
REPS = 16
N_REP = 16


def strengthened(drawn, rng, source, target, blocks, factor):
    def block_of(position):
        return (jnp.arange(drawn.shape[position]) // (drawn.shape[position] // blocks)).reshape((-1,) + (1,) * (drawn.ndim - 1 - position))

    near = jax.random.permutation(rng, blocks)[block_of(target)]
    second = (block_of(target) + blocks // 2) % blocks
    return jnp.where((block_of(source) == near) | (block_of(source) == second), factor * drawn, drawn)


def steps_of(key, dims, cuts, least, largest):
    def one(dim, parts):
        heights = jax.random.uniform(jax.random.fold_in(jax.random.fold_in(key, 6), dim), (parts,), jnp.float32, least / len(cuts), largest / len(cuts))
        return jnp.repeat(jnp.exp(heights), dims[dim] // parts).reshape((-1,) + (1,) * (len(dims) - dim - 1))

    factor_of = one(*cuts[0])
    for cut in cuts[1:]:
        factor_of = factor_of * one(*cut)
    return factor_of


def normal_values(key, extent, spread, most, pieces=(), held_as=jnp.bfloat16):
    values = jax.random.normal(key, extent, jnp.float32) * spread
    if len(pieces) > 0:
        values = steps_of(key, extent, pieces, -0.22, 0.18) * values
    return jnp.clip(values, min=-most, max=most).astype(held_as)


def noise_with(stream_key, shape, scale, bound, split, heavy, dtype=jnp.bfloat16):
    entries = scale * jax.random.normal(stream_key, shape, jnp.float32)
    if split:
        entries = entries * steps_of(stream_key, shape, split, -0.22, 0.18)
    return jnp.clip(strengthened(entries, jax.random.fold_in(stream_key, 3), *heavy), -bound, bound).astype(dtype)


def setup_inputs(seed: int = 0) -> dict:
    streams_of = jax.random.split(jax.random.key(seed), 6)
    activations = normal_values(streams_of[0], (REPS, TOK, D), 1.0, 6.0, ((0, 16), (1, 16)))
    cotangent = normal_values(streams_of[1], (REPS, TOK, FFW), (TOK ** -0.5), 0.13183594, ((0, 16), (2, 16)))
    drift = noise_with(streams_of[2], (REPS, D, FFW), 1.0, 8.0, ((0, 16), (2, 16)), (0, 1, 16, 2.0))
    outer_weights = normal_values(streams_of[3], (D, FFW), 1.0, 6.0, ((0, 256),), jnp.float32)
    momentum = normal_values(streams_of[4], (D, FFW), 1.0, 6.0, ((0, 256),), jnp.float32)
    return dict(activations=activations, cotangent=cotangent, drift=drift, outer_weights=outer_weights, momentum=momentum)


outer_rate = 0.7
nesterov = 0.9


def reference(activations, cotangent, drift, outer_weights, momentum):
    def per_group(total, items):
        acts, cot, own = items
        grad = jnp.dot(acts.T, cot, preferred_element_type=jnp.float32)
        delta = lax.optimization_barrier((own.astype(jnp.float32) + grad).astype(jnp.bfloat16))
        return total + delta.astype(jnp.float32), None

    start = jnp.zeros((drift.shape[1], drift.shape[2]), jnp.float32)
    summed, _ = lax.scan(per_group, start, (activations, cotangent, drift))
    average = summed / N_REP
    new_momentum = nesterov * momentum + average
    new_outer = outer_weights - outer_rate * (average + nesterov * new_momentum)
    weights = new_outer.astype(jnp.bfloat16)
    return weights, new_outer, new_momentum
```

```python
import functools

import jax
import jax.numpy as jnp
from jax import lax
from jax.experimental import pallas as pl
from jax.experimental.pallas import tpu as pltpu
from jax.sharding import PartitionSpec as P

outer_rate = 0.7
nesterov = 0.9

F32 = jnp.float32
BF16 = jnp.bfloat16
MESH = pl.DeviceIdType.MESH
N_SEND = 160
N_RECV = 160
N_LOCAL = 32


def kernel(at, cot, drift, outer, mom, wout, no_out, nm_out,
           abuf, cbuf, dbuf, pbuf, y1, y2, rbuf, zr, fbuf, xr, wsend, w1, obuf, mbuf,
           ss, rs, ls):
    rep = lax.axis_index("rep")
    tp = lax.axis_index("tp")
    y = rep // 4
    zhi = (rep // 2) % 2
    c = rep % 2
    x = tp // 4
    zlo = tp % 4
    z = zhi * 4 + zlo
    oc = 1 - c

    def dev(yy, zz, cc, xx):
        return ((yy % 4) * 4 + ((zz % 8) // 4) * 2 + cc, (xx % 4) * 4 + (zz % 4))

    counts = {"s": 0, "r": 0, "l": 0}
    sends = []

    def take(kind, n=1):
        base = counts[kind]
        counts[kind] += n
        return base

    def send(src, dst, to, rsem):
        copy = pltpu.make_async_remote_copy(
            src_ref=src, dst_ref=dst, send_sem=ss.at[take("s")], recv_sem=rs.at[rsem],
            device_id=to, device_id_type=MESH)
        copy.start()
        sends.append(copy)

    def arrive(ref, rsem):
        pltpu.make_async_copy(ref, ref, rs.at[rsem]).wait()

    def local(src, dst):
        copy = pltpu.make_async_copy(src, dst, ls.at[take("l")])
        copy.start()
        return copy

    partner = dev(y, z, oc, x)
    up, down = dev(y + 1, z, c, x), dev(y - 1, z, c, x)
    zup, zdown = dev(y, z + 1, c, x), dev(y, z - 1, c, x)

    greeted = [partner, up, down]
    greeted += [dev(y, z, cc, x + d) for d in (1, 3) for cc in (0, 1)]
    greeted += [dev(y, z, c, x + 2)]
    greeted += [dev(y, z + k, c, x) for k in range(1, 8)]
    barrier = pltpu.get_barrier_semaphore()
    for other in greeted:
        pl.semaphore_signal(barrier, inc=1, device_id=other, device_id_type=MESH)

    def lanes(group, xx):
        return pl.ds(pl.multiple_of((group * 4 + xx % 4) * 128, 128), 128)

    a_own = [local(at.at[:, c, r], abuf.at[r, :, :, lanes(c, x)]) for r in range(2)]
    c_own = local(cot.at[:, zlo], cbuf.at[zlo, c])
    d_own = [local(drift.at[:, c, r], dbuf.at[0, r]) for r in range(2)]
    o_own = local(outer, obuf)
    m_own = local(mom, mbuf)
    pl.semaphore_wait(barrier, len(greeted))

    a_part = take("r", 2)
    a_minus = take("r", 4)
    a_plus = take("r", 4)
    a_far = take("r", 4)
    c_part = take("r", 4)
    c_peer = take("r", 4)
    d_part = take("r", 2)

    def send_a(r):
        dst = abuf.at[r, :, :, lanes(c, x)]
        send(at.at[:, c, r], dst, dev(y, z, c, x + 1), a_minus + 2 * r + c)
        send(at.at[:, c, r], dst, dev(y, z, c, x - 1), a_plus + 2 * r + c)
        send(at.at[:, oc, r], dst, dev(y, z, oc, x + 1), a_minus + 2 * r + c)
        send(at.at[:, oc, r], dst, dev(y, z, oc, x - 1), a_plus + 2 * r + c)
        send(at.at[:, oc, r], dst, partner, a_part + r)

    def forward_a(r):
        for group in range(2):
            arrive(abuf.at[r, :, :, lanes(group, x - 1)], a_minus + 2 * r + group)
        src = abuf.at[r, :, :, lanes(0, x - 1)]
        send(src, src, dev(y, z, c, x + 1), a_far + 2 * r)
        for group in range(2):
            arrive(abuf.at[r, :, :, lanes(group, x + 1)], a_plus + 2 * r + group)
        src = abuf.at[r, :, :, lanes(1, x + 1)]
        send(src, src, dev(y, z, c, x - 1), a_far + 2 * r + 1)

    def finish_a(r):
        a_own[r].wait()
        arrive(abuf.at[r, :, :, lanes(oc, x)], a_part + r)
        for group in range(2):
            arrive(abuf.at[r, :, :, lanes(group, x + 2)], a_far + 2 * r + group)

    offsets = (0, 1, 3, 2)

    send_a(0)
    send(cot.at[:, zlo], cbuf.at[zlo, c], partner, c_part)
    send(drift.at[:, oc, 0], dbuf.at[1, 0], partner, d_part)
    for s in (1, 2, 3):
        to = (zlo - offsets[s]) % 4
        send(cot.at[:, to], cbuf.at[zlo, c], dev(y, zhi * 4 + to, c, x), c_peer + s)
    send_a(1)
    send(drift.at[:, oc, 1], dbuf.at[1, 1], partner, d_part + 1)

    def ready_c(s):
        q = (zlo + offsets[s]) % 4
        if s == 0:
            c_own.wait()
        else:
            arrive(cbuf.at[q, c], c_peer + s)
            send(cbuf.at[q, c], cbuf.at[q, c], partner, c_part + s)
        arrive(cbuf.at[q, oc], c_part + s)

    y_first = take("r", 16)
    y_plain = take("r", 16)
    y_sum = take("r", 16)

    def compute(r, s):
        unit = r * 4 + s
        q = (zlo + offsets[s]) % 4
        if r == 0:
            ready_c(s)
        if s == 0:
            d_own[r].wait()
            arrive(dbuf.at[1, r], d_part + r)

        def piece(j, carry):
            yy = (y + j) % 4
            lhs = abuf[r, pl.ds(yy * 2, 2)].reshape(256, 1024)
            rhs = cbuf[q].reshape(1024, 512)
            total = jnp.dot(lhs, rhs, preferred_element_type=F32)
            if s == 0:
                total = total + dbuf[0, r, pl.ds(yy * 2, 2)].reshape(256, 512).astype(F32)
                total = total + dbuf[1, r, pl.ds(yy * 2, 2)].reshape(256, 512).astype(F32)
            pbuf[r, s, j] = total.astype(BF16)
            return carry

        lax.fori_loop(0, 4, piece, 0)
        low, high = pl.ds(0, 128), pl.ds(128, 128)
        send(pbuf.at[r, s, 2, low], y1.at[0, r, s], up, y_first + unit)
        send(pbuf.at[r, s, 2, high], y1.at[1, r, s], down, y_first + 8 + unit)
        send(pbuf.at[r, s, 1, high], y2.at[0, r, s, high], up, y_plain + unit)
        send(pbuf.at[r, s, 3, low], y2.at[1, r, s, low], down, y_plain + 8 + unit)

    def relay_y(r, s):
        unit = r * 4 + s
        low, high = pl.ds(0, 128), pl.ds(128, 128)
        arrive(y1.at[0, r, s], y_first + unit)
        pbuf[r, s, 1, low] = (pbuf[r, s, 1, low].astype(F32) + y1[0, r, s].astype(F32)).astype(BF16)
        send(pbuf.at[r, s, 1, low], y2.at[0, r, s, low], up, y_sum + unit)
        arrive(y1.at[1, r, s], y_first + 8 + unit)
        pbuf[r, s, 3, high] = (pbuf[r, s, 3, high].astype(F32) + y1[1, r, s].astype(F32)).astype(BF16)
        send(pbuf.at[r, s, 3, high], y2.at[1, r, s, high], down, y_sum + 8 + unit)

    def finish_y(r, s):
        unit = r * 4 + s
        q = (zlo + offsets[s]) % 4
        low, high = pl.ds(0, 128), pl.ds(128, 128)
        arrive(y2.at[0, r, s, high], y_plain + unit)
        arrive(y2.at[1, r, s, low], y_plain + 8 + unit)
        arrive(y2.at[0, r, s, low], y_sum + unit)
        arrive(y2.at[1, r, s, high], y_sum + 8 + unit)
        for hi in range(2):
            for px in range(2):
                for pz in range(4):
                    rows = pl.ds(hi * 128 + px * 64 + pz * 16, 16)
                    total = (pbuf[r, s, 0, rows].astype(F32) + y2[0, r, s, rows].astype(F32)
                             + y2[1, r, s, rows].astype(F32))
                    rbuf[r, hi * 4 + pz, q, px] = total.astype(BF16)

    z_up = take("r", 8)
    z_down = take("r", 8)

    def ring_z(r, step):
        lo, hi = pl.ds(0, 2), pl.ds(2, 2)
        if step == 0:
            far = (z + 4) % 8
            send(rbuf.at[r, far, lo], zr.at[0, r, 0, lo], zup, z_up + 4 * r)
            send(rbuf.at[r, far, hi], zr.at[1, r, 0, hi], zdown, z_down + 4 * r)
            return
        last = step == 4
        for way, (base, to) in enumerate(((z_up, zup), (z_down, zdown))):
            part = (lo, hi)[way] if step == 1 else pl.ds(0, 4)
            arrive(zr.at[way, r, step - 1, part], base + 4 * r + step - 1)
            if not last:
                target = (z + (4 - step)) % 8 if way == 0 else (z + 4 + step) % 8
                rbuf[r, target, part] = (rbuf[r, target, part].astype(F32)
                                         + zr[way, r, step - 1, part].astype(F32)).astype(BF16)
                send(rbuf.at[r, target], zr.at[way, r, step], to, base + 4 * r + step)
        if last:
            for q in range(4):
                for px in range(2):
                    total = (rbuf[r, z, q, px].astype(F32) + zr[0, r, 3, q, px].astype(F32)
                             + zr[1, r, 3, q, px].astype(F32))
                    fbuf[2 * r + px, q] = total.astype(BF16)

    forward_a(0)
    finish_a(0)
    compute(0, 0)
    compute(0, 1)
    relay_y(0, 0)
    compute(0, 2)
    relay_y(0, 1)
    forward_a(1)
    finish_y(0, 0)
    compute(0, 3)
    relay_y(0, 2)
    finish_y(0, 1)
    finish_a(1)
    compute(1, 0)
    relay_y(0, 3)
    finish_y(0, 2)
    compute(1, 1)
    relay_y(1, 0)
    finish_y(0, 3)
    ring_z(0, 0)
    compute(1, 2)
    relay_y(1, 1)
    finish_y(1, 0)
    ring_z(0, 1)
    compute(1, 3)
    relay_y(1, 2)
    finish_y(1, 1)
    ring_z(0, 2)
    relay_y(1, 3)
    finish_y(1, 2)
    ring_z(0, 3)
    finish_y(1, 3)
    ring_z(1, 0)
    ring_z(0, 4)
    for step in range(1, 5):
        ring_z(1, step)

    x_in = take("r", 4)
    for d in (1, 3, 2):
        xx = (x + d) % 4
        send(fbuf.at[xx], xr.at[x], dev(y, z, c, xx), x_in + d)
    xr[x] = fbuf[x]
    o_own.wait()
    m_own.wait()
    for d in (1, 3, 2):
        arrive(xr.at[(x - d) % 4], x_in + d)

    for xx in range(4):
        for q in range(4):
            cols = pl.ds((xx * 4 + q) * 512, 512)
            average = xr[xx, q].astype(F32) / 16
            momentum = nesterov * mbuf[:, cols] + average
            weights = obuf[:, cols] - outer_rate * (average + nesterov * momentum)
            mbuf[:, cols] = momentum
            obuf[:, cols] = weights
            wsend[xx, q] = weights.astype(BF16)

    r_one = take("r", 4)
    for d in (1, 3, 2):
        xx = (x + d) % 4
        send(wsend.at[xx], w1.at[x], dev(y, z, c, xx), r_one + d)
    w1[x] = wsend[x]
    o_done = local(obuf, no_out)
    m_done = local(mbuf, nm_out)
    for d in (1, 3, 2):
        arrive(w1.at[(x - d) % 4], r_one + d)

    r_two = take("r", 8)
    own = wout.at[rep, :, zlo]
    for k in (4, 3, 5, 2, 6, 1, 7):
        zz = (z + k) % 8
        send(w1.at[:, zz % 4], own, dev(y, zz, c, x), r_two + k)
    own_done = local(w1.at[:, zlo], own)

    def block(yy, half, cc):
        return wout.at[(yy % 4) * 4 + 2 * half + cc]

    r_up = take("r", 2)
    r_down = take("r", 2)
    r_far = take("r", 2)
    r_part = take("r", 8)
    own_done.wait()
    for k in (1, 7, 2, 6, 3, 5, 4):
        zz = (z - k) % 8
        arrive(wout.at[y * 4 + (zz // 4) * 2 + c, :, zz % 4], r_two + k)
    for half in range(2):
        src = block(y, half, c)
        send(src, src, up, r_down + half)
        send(src, src, down, r_up + half)
    for half in range(2):
        src = block(y, half, c)
        send(src, src, partner, r_part + half)
    for half in range(2):
        src = block(y - 1, half, c)
        arrive(src, r_down + half)
        if half == 0:
            send(src, src, up, r_far)
        send(src, src, partner, r_part + 2 + half)
        half = 1 - half
        src = block(y + 1, half, c)
        arrive(src, r_up + half)
        if half == 1:
            send(src, src, down, r_far + 1)
        send(src, src, partner, r_part + 4 + half)
    for half in range(2):
        src = block(y + 2, half, c)
        arrive(src, r_far + half)
        send(src, src, partner, r_part + 6 + half)
    for half in range(2):
        arrive(block(y, half, oc), r_part + half)
        arrive(block(y - 1, half, oc), r_part + 2 + half)
        arrive(block(y + 1, half, oc), r_part + 4 + half)
        arrive(block(y + 2, half, oc), r_part + 6 + half)
    o_done.wait()
    m_done.wait()
    for copy in sends:
        copy.wait_send()


def on_device(activations, cotangent, drift, outer_weights, momentum):
    at = activations[0].T.reshape(8, 2, 2, 128, 128)
    cot = cotangent[0].reshape(4, 4, 128, 512)
    dr = drift[0].reshape(8, 2, 2, 128, 512)
    any_spec = pl.BlockSpec(memory_space=pl.ANY)
    weights, new_outer, new_momentum = pl.pallas_call(
        kernel,
        out_shape=(
            jax.ShapeDtypeStruct((16, 4, 4, 16, 512), BF16),
            jax.ShapeDtypeStruct((16, 8192), F32),
            jax.ShapeDtypeStruct((16, 8192), F32),
        ),
        in_specs=[any_spec] * 5,
        out_specs=[any_spec] * 3,
        scratch_shapes=[
            pltpu.VMEM((2, 8, 128, 1024), BF16),
            pltpu.VMEM((4, 2, 4, 128, 512), BF16),
            pltpu.VMEM((2, 2, 8, 128, 512), BF16),
            pltpu.VMEM((2, 4, 4, 256, 512), BF16),
            pltpu.VMEM((2, 2, 4, 128, 512), BF16),
            pltpu.VMEM((2, 2, 4, 256, 512), BF16),
            pltpu.VMEM((2, 8, 4, 2, 16, 512), BF16),
            pltpu.VMEM((2, 2, 4, 4, 2, 16, 512), BF16),
            pltpu.VMEM((4, 4, 16, 512), BF16),
            pltpu.VMEM((4, 4, 16, 512), BF16),
            pltpu.VMEM((4, 4, 16, 512), BF16),
            pltpu.VMEM((4, 4, 16, 512), BF16),
            pltpu.VMEM((16, 8192), F32),
            pltpu.VMEM((16, 8192), F32),
            pltpu.SemaphoreType.DMA((N_SEND,)),
            pltpu.SemaphoreType.DMA((N_RECV,)),
            pltpu.SemaphoreType.DMA((N_LOCAL,)),
        ],
        compiler_params=pltpu.CompilerParams(
            collective_id=0, has_side_effects=True, vmem_limit_bytes=60 * 1024 * 1024
        ),
        name="outer_step",
    )(at, cot, dr, outer_weights, momentum)
    return weights.reshape(4096, 512), new_outer, new_momentum


def solution(mesh):
    in_specs = (
        P("rep", "tp", None),
        P("rep", None, "tp"),
        P("rep", None, "tp"),
        P(("rep", "tp"), None),
        P(("rep", "tp"), None),
    )
    out_specs = (P(None, "tp"), P(("rep", "tp"), None), P(("rep", "tp"), None))
    return jax.shard_map(
        on_device, mesh=mesh, in_specs=in_specs, out_specs=out_specs, check_vma=False
    )
```

```python
import functools

import jax
import jax.numpy as jnp
from jax import lax
from jax.experimental import pallas as pl
from jax.experimental.pallas import tpu as pltpu
from jax.sharding import PartitionSpec as P

outer_rate = 0.7
nesterov = 0.9

F32 = jnp.float32
BF16 = jnp.bfloat16
MESH = pl.DeviceIdType.MESH
N_SEND = 288
N_RECV = 304
N_LOCAL = 32


def kernel(act, cot, drift, outer, mom, wout, no_out, nm_out,
           av, atv, abuf, cbuf, dbuf, pbuf, y1, y2, rbuf, zr, wbuf, obuf, mbuf,
           ss, rs, ls):
    rep = lax.axis_index("rep")
    tp = lax.axis_index("tp")
    y = rep // 4
    zhi = (rep // 2) % 2
    c = rep % 2
    x = tp // 4
    zlo = tp % 4
    z = zhi * 4 + zlo
    oc = 1 - c

    def dev(yy, zz, cc, xx):
        return ((yy % 4) * 4 + ((zz % 8) // 4) * 2 + cc, (xx % 4) * 4 + (zz % 4))

    counts = {"s": 0, "r": 0, "l": 0}
    sends = []

    def take(kind, n=1):
        base = counts[kind]
        counts[kind] += n
        return base

    def remote(src, dst, to, rsem):
        return pltpu.make_async_remote_copy(
            src_ref=src, dst_ref=dst, send_sem=ss.at[take("s")], recv_sem=rs.at[rsem],
            device_id=to, device_id_type=MESH)

    def send(src, dst, to, rsem):
        copy = remote(src, dst, to, rsem)
        copy.start()
        sends.append(copy.wait_send)

    def arrive(ref, rsem):
        pltpu.make_async_copy(ref, ref, rs.at[rsem]).wait()

    def local(src, dst):
        copy = pltpu.make_async_copy(src, dst, ls.at[take("l")])
        copy.start()
        return copy

    partner = dev(y, z, oc, x)
    up, down = dev(y + 1, z, c, x), dev(y - 1, z, c, x)
    zup, zdown = dev(y, z + 1, c, x), dev(y, z - 1, c, x)

    greeted = [dev(y, z + k, c, x) for k in (4, 3, 5, 2, 6, 1, 7)]
    greeted += [dev(y, z, c, x + 2)]
    greeted += [dev(y, z, cc, x + d) for d in (1, 3) for cc in (0, 1)]
    greeted += [up, down, partner]
    barrier = pltpu.get_barrier_semaphore()
    for other in greeted:
        pl.semaphore_signal(barrier, inc=1, device_id=other, device_id_type=MESH)

    def lanes(group, xx):
        return pl.ds(pl.multiple_of((group * 4 + xx % 4) * 128, 128), 128)

    def columns(xx):
        return pl.ds(pl.multiple_of((xx % 4) * 2048, 2048), 2048)

    a_in = local(act, av)
    c_own = local(cot.at[:, zlo], cbuf.at[zlo, c])
    d_own = local(drift.at[:, c], dbuf.at[0])
    o_own = local(outer.at[:, columns(x)], obuf.at[x])
    m_own = local(mom.at[:, columns(x)], mbuf.at[x])
    a_in.wait()
    for j in range(32):
        tile = av[:, pl.ds(j * 128, 128)].T
        for i in range(2):
            atv[j // 4, (j // 2) % 2, 2 * (j % 2) + i] = tile[i * 64:(i + 1) * 64]
    pl.semaphore_wait(barrier, len(greeted))

    a_part = take("r", 4)
    a_minus = take("r", 8)
    a_plus = take("r", 8)
    a_far = take("r", 8)
    c_part = take("r", 4)
    c_peer = take("r", 4)
    d_part = take("r", 1)
    a_own = []

    def send_a(r):
        dst = abuf.at[r, :, :, lanes(c, x)]
        send(atv.at[:, c, r], dst, dev(y, z, c, x + 1), a_minus + 2 * r + c)
        send(atv.at[:, c, r], dst, dev(y, z, c, x - 1), a_plus + 2 * r + c)
        send(atv.at[:, oc, r], dst, dev(y, z, oc, x + 1), a_minus + 2 * r + c)
        send(atv.at[:, oc, r], dst, dev(y, z, oc, x - 1), a_plus + 2 * r + c)
        send(atv.at[:, oc, r], dst, partner, a_part + r)
        a_own.append(local(atv.at[:, c, r], dst))

    def forward_a(r):
        for group in range(2):
            arrive(abuf.at[r, :, :, lanes(group, x - 1)], a_minus + 2 * r + group)
        src = abuf.at[r, :, :, lanes(0, x - 1)]
        send(src, src, dev(y, z, c, x + 1), a_far + 2 * r)
        for group in range(2):
            arrive(abuf.at[r, :, :, lanes(group, x + 1)], a_plus + 2 * r + group)
        src = abuf.at[r, :, :, lanes(1, x + 1)]
        send(src, src, dev(y, z, c, x - 1), a_far + 2 * r + 1)

    def finish_a(r):
        a_own[r].wait()
        arrive(abuf.at[r, :, :, lanes(oc, x)], a_part + r)
        for group in range(2):
            arrive(abuf.at[r, :, :, lanes(group, x + 2)], a_far + 2 * r + group)

    def block_of(s, at=None):
        at = zlo if at is None else at
        pair = at // 2
        low = at % 2
        return (at, 2 * pair + 1 - low, 3 - at, 2 * (1 - pair) + low)[s]

    def send_c(s):
        if s == 0:
            send(cot.at[:, zlo], cbuf.at[zlo, c], partner, c_part)
        else:
            to = block_of(s)
            send(cot.at[:, to], cbuf.at[zlo, c], dev(y, zhi * 4 + to, c, x), c_peer + s)

    def send_d():
        send(drift.at[:, oc], dbuf.at[1], partner, d_part)

    def ready_c(s):
        q = block_of(s)
        if s == 0:
            c_own.wait()
        else:
            arrive(cbuf.at[q, c], c_peer + s)
            send(cbuf.at[q, c], cbuf.at[q, c], partner, c_part + s)
        arrive(cbuf.at[q, oc], c_part + s)

    y_first = take("r", 32)
    y_plain = take("r", 32)
    y_sum = take("r", 32)

    def compute(r, s):
        unit = r * 4 + s
        q = block_of(s)
        if r == 0:
            ready_c(s)
        if r == 0 and s == 0:
            d_own.wait()
            arrive(dbuf.at[1], d_part)
        lhs = abuf[r].reshape(512, 1024)
        rhs = cbuf[q].reshape(1024, 512)
        total = jnp.dot(lhs, rhs, preferred_element_type=F32)
        if s == 0:
            total = total + dbuf[0, :, r].reshape(512, 512).astype(F32)
            total = total + dbuf[1, :, r].reshape(512, 512).astype(F32)
        pbuf[r, s] = total.astype(BF16).reshape(4, 2, 64, 512)
        far, near, back = (y + 2) % 4, (y + 1) % 4, (y + 3) % 4
        send(pbuf.at[r, s, far, 0], y1.at[0, r, s], up, y_first + unit)
        send(pbuf.at[r, s, far, 1], y1.at[1, r, s], down, y_first + 16 + unit)
        send(pbuf.at[r, s, near, 1], y2.at[0, r, s, 1], up, y_plain + unit)
        send(pbuf.at[r, s, back, 0], y2.at[1, r, s, 0], down, y_plain + 16 + unit)

    def relay_y(r, s):
        unit = r * 4 + s
        near, back = (y + 1) % 4, (y + 3) % 4
        arrive(y1.at[0, r, s], y_first + unit)
        pbuf[r, s, near, 0] = (pbuf[r, s, near, 0].astype(F32) + y1[0, r, s].astype(F32)).astype(BF16)
        send(pbuf.at[r, s, near, 0], y2.at[0, r, s, 0], up, y_sum + unit)
        arrive(y1.at[1, r, s], y_first + 16 + unit)
        pbuf[r, s, back, 1] = (pbuf[r, s, back, 1].astype(F32) + y1[1, r, s].astype(F32)).astype(BF16)
        send(pbuf.at[r, s, back, 1], y2.at[1, r, s, 1], down, y_sum + 16 + unit)

    def finish_y(r, s):
        unit = r * 4 + s
        q = block_of(s)
        arrive(y2.at[0, r, s, 1], y_plain + unit)
        arrive(y2.at[1, r, s, 0], y_plain + 16 + unit)
        arrive(y2.at[0, r, s, 0], y_sum + unit)
        arrive(y2.at[1, r, s, 1], y_sum + 16 + unit)
        for hi in range(2):
            total = (pbuf[r, s, y, hi].astype(F32) + y2[0, r, s, hi].astype(F32)
                     + y2[1, r, s, hi].astype(F32)).astype(BF16)
            for pz in range(4):
                rbuf[r, hi * 4 + pz, q] = total[pz * 16:(pz + 1) * 16]

    z_up = take("r", 16)
    z_down = take("r", 16)

    def ring_z(r, step):
        lo, hi = pl.ds(0, 2), pl.ds(2, 2)
        if step == 0:
            far = (z + 4) % 8
            send(rbuf.at[r, far, lo], zr.at[0, r, 0, lo], zup, z_up + 4 * r)
            send(rbuf.at[r, far, hi], zr.at[1, r, 0, hi], zdown, z_down + 4 * r)
            return
        for way, (base, to) in enumerate(((z_up, zup), (z_down, zdown))):
            part = (lo, hi)[way] if step == 1 else pl.ds(0, 4)
            arrive(zr.at[way, r, step - 1, part], base + 4 * r + step - 1)
            if step < 4:
                target = (z + (4 - step)) % 8 if way == 0 else (z + 4 + step) % 8
                rbuf[r, target, part] = (rbuf[r, target, part].astype(F32)
                                         + zr[way, r, step - 1, part].astype(F32)).astype(BF16)
                send(rbuf.at[r, target], zr.at[way, r, step], to, base + 4 * r + step)

    def skip_z(step):
        halves = pl.ds(0, 2), pl.ds(2, 2)
        for way, base in enumerate((z_up, z_down)):
            sign = 1 - 2 * way
            one, two = (z + 8 + sign) % 8, (z + 8 + 2 * sign) % 8
            half = halves[way]
            if step == 0:
                to = dev(y, two, c, x)
                send(rbuf.at[3, (z + 4) % 8, half], zr.at[way, 3, 0, half], to, base + 12)
                send(rbuf.at[3, (z + 8 + 3 * sign) % 8], zr.at[way, 3, 1], to, base + 13)
            elif step == 1:
                arrive(zr.at[way, 3, 0, half], base + 12)
                rbuf[3, two, half] = (rbuf[3, two, half].astype(F32)
                                      + zr[way, 3, 0, half].astype(F32)).astype(BF16)
                send(rbuf.at[3, two], zr.at[way, 3, 2], dev(y, two, c, x), base + 14)
                arrive(zr.at[way, 3, 1], base + 13)
                rbuf[3, one] = (rbuf[3, one].astype(F32)
                                + zr[way, 3, 1].astype(F32)).astype(BF16)
                send(rbuf.at[3, one], zr.at[way, 3, 3], dev(y, one, c, x), base + 15)
            else:
                arrive(zr.at[way, 3, 2], base + 14)
                arrive(zr.at[way, 3, 3], base + 15)

    s_out = take("r", 4)
    s_mom = take("r", 4)

    def send_state():
        for d in (1, 3, 2):
            xx = (x + d) % 4
            send(outer.at[:, columns(xx)], obuf.at[x], dev(y, z, c, xx), s_out + d)
            send(mom.at[:, columns(xx)], mbuf.at[x], dev(y, z, c, xx), s_mom + d)

    def finish_state():
        o_own.wait()
        m_own.wait()
        for d in (1, 3, 2):
            arrive(obuf.at[(x - d) % 4], s_out + d)
            arrive(mbuf.at[(x - d) % 4], s_mom + d)

    b_out = take("r", 4)
    b_mom = take("r", 4)
    r_two = take("r", 32)
    w_own = []

    def update(r):
        for q in range(4):
            cols = pl.ds(q * 512, 512)
            total = rbuf[r, z, q].astype(F32)
            for way in range(2):
                for step in ((3,), (2, 3))[r == 3]:
                    total = total + zr[way, r, step, q].astype(F32)
            average = total / 16
            momentum = nesterov * mbuf[r, :, cols] + average
            weights = obuf[r, :, cols] - outer_rate * (average + nesterov * momentum)
            mbuf[r, :, cols] = momentum
            obuf[r, :, cols] = weights
            wbuf[r, q] = weights.astype(BF16)
        own = wout.at[y, zhi, c, r, zlo]
        for k in (4, 3, 5, 2, 6, 1, 7):
            zz = (z + k) % 8
            send(wbuf.at[r, zz % 4], own, dev(y, zz, c, x), r_two + 8 * r + k)
        w_own.append(local(wbuf.at[r, zlo], own))
        backs = [remote(buf.at[r], out.at[:, columns(x)], dev(y, z, c, r), base + x)
                 for buf, out, base in ((obuf, no_out, b_out), (mbuf, nm_out, b_mom))]
        keeps = [pltpu.make_async_copy(buf.at[r], out.at[:, columns(x)], ls.at[take("l")])
                 for buf, out in ((obuf, no_out), (mbuf, nm_out))]

        @pl.when(x != r)
        def _():
            for copy in backs:
                copy.start()

        @pl.when(x == r)
        def _():
            for copy in keeps:
                copy.start()

        def finish():
            @pl.when(x != r)
            def _():
                for copy in backs:
                    copy.wait_send()

            @pl.when(x == r)
            def _():
                for copy in keeps:
                    copy.wait()

        sends.append(finish)

    r_up = take("r", 4)
    r_down = take("r", 4)
    r_far = take("r", 8)
    r_part = take("r", 20)

    def gather_own(r):
        w_own[r].wait()
        for k in (1, 7, 2, 6, 3, 5, 4):
            zz = (z - k) % 8
            arrive(wout.at[y, zz // 4, c, r, zz % 4], r_two + 8 * r + k)
        src = wout.at[y, :, c, r]
        send(src, src, up, r_down + r)
        send(src, src, down, r_up + r)
        send(src, src, partner, r_part + 5 * r)

    def gather_near(r):
        back, near = (y + 3) % 4, (y + 1) % 4
        src = wout.at[back, :, c, r]
        arrive(src, r_down + r)
        send(wout.at[back, 0, c, r], wout.at[back, 0, c, r], up, r_far + 2 * r)
        send(src, src, partner, r_part + 5 * r + 1)
        src = wout.at[near, :, c, r]
        arrive(src, r_up + r)
        send(wout.at[near, 1, c, r], wout.at[near, 1, c, r], down, r_far + 2 * r + 1)
        send(src, src, partner, r_part + 5 * r + 2)

    def gather_far(r):
        for half in range(2):
            src = wout.at[(y + 2) % 4, half, c, r]
            arrive(src, r_far + 2 * r + half)
            send(src, src, partner, r_part + 5 * r + 3 + half)

    def gather_done(r):
        arrive(wout.at[y, :, oc, r], r_part + 5 * r)
        arrive(wout.at[(y + 3) % 4, :, oc, r], r_part + 5 * r + 1)
        arrive(wout.at[(y + 1) % 4, :, oc, r], r_part + 5 * r + 2)
        for half in range(2):
            arrive(wout.at[(y + 2) % 4, half, oc, r], r_part + 5 * r + 3 + half)

    send_a(0)
    send_c(0)
    send_c(1)
    send_c(2)
    send_d()
    forward_a(0)
    send_a(1)
    finish_a(0)

    units = ((0, 0), (0, 1), (1, 0), (1, 1), (0, 2), (1, 2), (2, 0), (2, 1),
             (2, 2), (0, 3), (1, 3), (2, 3), (3, 0), (3, 1), (3, 2), (3, 3))

    def slot(i):
        if 1 <= i < 17:
            relay_y(*units[i - 1])
        if 3 <= i:
            finish_y(*units[i - 3])

    compute(0, 0)
    compute(0, 1)
    slot(1)
    forward_a(1)
    send_a(2)
    finish_a(1)
    send_c(3)
    compute(1, 0)
    slot(2)
    compute(1, 1)
    slot(3)
    compute(0, 2)
    forward_a(2)
    send_a(3)
    send_state()
    slot(4)
    compute(1, 2)
    slot(5)
    finish_a(2)
    compute(2, 0)
    slot(6)
    compute(2, 1)
    slot(7)
    forward_a(3)
    compute(2, 2)
    slot(8)
    compute(0, 3)
    relay_y(2, 2)
    finish_y(2, 0)
    compute(1, 3)
    relay_y(0, 3)
    finish_y(2, 1)
    compute(2, 3)
    finish_a(3)
    compute(3, 0)
    relay_y(1, 3)
    finish_y(2, 2)
    finish_y(0, 3)
    ring_z(0, 0)
    compute(3, 1)
    relay_y(2, 3)
    finish_y(1, 3)
    ring_z(1, 0)
    ring_z(0, 1)
    compute(3, 2)
    relay_y(3, 0)
    finish_y(2, 3)
    ring_z(2, 0)
    ring_z(0, 2)
    ring_z(1, 1)
    compute(3, 3)
    relay_y(3, 1)
    finish_y(3, 0)
    ring_z(0, 3)
    ring_z(1, 2)
    ring_z(2, 1)
    relay_y(3, 2)
    finish_y(3, 1)
    ring_z(0, 4)
    finish_state()
    update(0)
    ring_z(1, 3)
    ring_z(2, 2)
    relay_y(3, 3)
    finish_y(3, 2)
    ring_z(1, 4)
    update(1)
    ring_z(2, 3)
    finish_y(3, 3)
    skip_z(0)
    ring_z(2, 4)
    update(2)
    gather_own(0)
    gather_own(1)
    skip_z(1)
    gather_near(0)
    gather_near(1)
    gather_own(2)
    skip_z(2)
    update(3)
    gather_far(0)
    gather_far(1)
    gather_near(2)
    gather_own(3)
    gather_far(2)
    gather_done(0)
    gather_done(1)
    gather_near(3)
    gather_done(2)
    gather_far(3)
    gather_done(3)
    for d in (1, 3, 2):
        xx = (x - d) % 4
        arrive(no_out.at[:, columns(xx)], b_out + xx)
        arrive(nm_out.at[:, columns(xx)], b_mom + xx)
    for finish in sends:
        finish()


def on_device(activations, cotangent, drift, outer_weights, momentum):
    cot = cotangent[0].reshape(4, 4, 128, 512)
    dr = drift[0].reshape(8, 2, 4, 64, 512)
    any_spec = pl.BlockSpec(memory_space=pl.ANY)
    hbm_spec = pl.BlockSpec(memory_space=pltpu.HBM)
    weights, new_outer, new_momentum = pl.pallas_call(
        kernel,
        out_shape=(
            pltpu.VMEM((4, 2, 2, 4, 4, 16, 512), BF16),
            pltpu.VMEM((16, 8192), F32),
            pltpu.VMEM((16, 8192), F32),
        ),
        in_specs=[hbm_spec] * 5,
        out_specs=[any_spec] * 3,
        scratch_shapes=[
            pltpu.VMEM((128, 4096), BF16),
            pltpu.VMEM((8, 2, 4, 64, 128), BF16),
            pltpu.VMEM((4, 8, 64, 1024), BF16),
            pltpu.VMEM((4, 2, 4, 128, 512), BF16),
            pltpu.VMEM((2, 8, 4, 64, 512), BF16),
            pltpu.VMEM((4, 4, 4, 2, 64, 512), BF16),
            pltpu.VMEM((2, 4, 4, 64, 512), BF16),
            pltpu.VMEM((2, 4, 4, 2, 64, 512), BF16),
            pltpu.VMEM((4, 8, 4, 16, 512), BF16),
            pltpu.VMEM((2, 4, 4, 4, 16, 512), BF16),
            pltpu.VMEM((4, 4, 16, 512), BF16),
            pltpu.VMEM((4, 16, 2048), F32),
            pltpu.VMEM((4, 16, 2048), F32),
            pltpu.SemaphoreType.DMA((N_SEND,)),
            pltpu.SemaphoreType.DMA((N_RECV,)),
            pltpu.SemaphoreType.DMA((N_LOCAL,)),
        ],
        compiler_params=pltpu.CompilerParams(
            collective_id=0, has_side_effects=True, vmem_limit_bytes=54 * 1024 * 1024
        ),
        name="outer_step",
    )(activations[0], cot, dr, outer_weights, momentum)
    return weights.reshape(4096, 512), new_outer, new_momentum


def solution(mesh):
    in_specs = (
        P("rep", "tp", None),
        P("rep", None, "tp"),
        P("rep", None, "tp"),
        P(("rep", "tp"), None),
        P(("rep", "tp"), None),
    )
    out_specs = (P(None, "tp"), P(("rep", "tp"), None), P(("rep", "tp"), None))
    return jax.shard_map(
        on_device, mesh=mesh, in_specs=in_specs, out_specs=out_specs, check_vma=False
    )
```

```python
import functools

import jax
import jax.numpy as jnp
from jax import lax
from jax.experimental import pallas as pl
from jax.experimental.pallas import tpu as pltpu
from jax.sharding import PartitionSpec as P

outer_rate = 0.7
nesterov = 0.9

F32 = jnp.float32
BF16 = jnp.bfloat16
MESH = pl.DeviceIdType.MESH
POOL = 72
N_RECV = 192
N_LOCAL = 16

ACTS = (12.5, 23.5, 35.0, 47.0)
COTS = ((1.0, 13.0, 16.0, 28.0), (1.0, 24.0, 41.0, 50.0))
PACE = 2.08


def reduction_order():
    waiting = [(h * 4 + r, s, max(ACTS[r], COTS[h][s]))
               for h in range(2) for r in range(4) for s in range(4)]
    now, order = 0.0, []
    while waiting:
        now = max(now, min(ready for _, _, ready in waiting))
        unit = next(u for u in waiting if u[2] <= now)
        waiting.remove(unit)
        order.append((unit[0], unit[1], unit[2], now))
        now += PACE
    return order


def kernel(act, cot, drift, outer, mom, wout, no_out, nm_out,
           av, atv, abuf, cbuf, dbuf, pbuf, y1, y2, rbuf, zr, wbuf, obuf, mbuf, tloc, tbuf, fbuf, xr,
           ss, rs, ls):
    rep = lax.axis_index("rep")
    tp = lax.axis_index("tp")
    y = rep // 4
    zhi = (rep // 2) % 2
    c = rep % 2
    x = tp // 4
    zlo = tp % 4
    z = zhi * 4 + zlo
    oc = 1 - c

    def dev(yy, zz, cc, xx):
        return ((yy % 4) * 4 + ((zz % 8) // 4) * 2 + cc, (xx % 4) * 4 + (zz % 4))

    counts = {"s": 0, "r": 0, "l": 0}
    sends = []

    def take(kind, n=1):
        base = counts[kind]
        counts[kind] += n
        return base

    def remote(src, dst, to, rsem, ssem):
        return pltpu.make_async_remote_copy(
            src_ref=src, dst_ref=dst, send_sem=ss.at[ssem], recv_sem=rs.at[rsem],
            device_id=to, device_id_type=MESH)

    def send(src, dst, to, rsem):
        if len(sends) == POOL:
            sends.pop(0)()
        copy = remote(src, dst, to, rsem, take("s") % POOL)
        copy.start()
        sends.append(copy.wait_send)

    def arrive(ref, rsem):
        pltpu.make_async_copy(ref, ref, rs.at[rsem]).wait()

    def local(src, dst):
        copy = pltpu.make_async_copy(src, dst, ls.at[take("l")])
        copy.start()
        return copy

    partner = dev(y, z, oc, x)
    up, down = dev(y + 1, z, c, x), dev(y - 1, z, c, x)
    zup, zdown = dev(y, z + 1, c, x), dev(y, z - 1, c, x)

    greeted = [dev(y, z + k, c, x) for k in (4, 3, 5, 2, 6, 1, 7)]
    greeted += [dev(y, z, c, x + 2)]
    greeted += [dev(y, z, cc, x + d) for d in (1, 3) for cc in (0, 1)]
    greeted += [up, down, partner]
    barrier = pltpu.get_barrier_semaphore()
    for other in greeted:
        pl.semaphore_signal(barrier, inc=1, device_id=other, device_id_type=MESH)

    def lanes(group, xx):
        return pl.ds(pl.multiple_of((group * 4 + xx % 4) * 128, 128), 128)

    def columns(xx):
        return pl.ds(pl.multiple_of((xx % 4) * 2048, 2048), 2048)

    a_in = local(act, av)
    c_own = local(cot.at[:, zlo], cbuf.at[zlo, c])
    d_own = local(drift.at[:, c], dbuf.at[0])
    o_own = local(outer, obuf)
    m_own = local(mom, mbuf)
    a_in.wait()
    for j in range(32):
        tile = av[:, pl.ds(j * 128, 128)].T
        for i in range(2):
            atv[j // 4, (j // 2) % 2, 2 * (j % 2) + i] = tile[i * 64:(i + 1) * 64]
    pl.semaphore_wait(barrier, len(greeted))

    a_part = take("r", 4)
    a_minus = take("r", 8)
    a_plus = take("r", 8)
    a_far = take("r", 8)
    c_part = take("r", 8)
    c_peer = take("r", 8)
    d_part = take("r", 1)
    a_own = []

    def send_a(r):
        dst = abuf.at[r, :, :, lanes(c, x)]
        for turn in range(2):
            ahead = 1 - 2 * c if turn == 0 else 2 * c - 1
            rsem = a_minus + 2 * r + c + 8 * (c if turn == 0 else oc)
            send(atv.at[:, c, r], dst, dev(y, z, c, x + 4 + ahead), rsem)
            send(atv.at[:, oc, r], dst, dev(y, z, oc, x + 4 + ahead), rsem)
        send(atv.at[:, oc, r], dst, partner, a_part + r)
        a_own.append(local(atv.at[:, c, r], dst))

    def forward_a(r):
        src = abuf.at[r, :, :, lanes(0, x + 3)]
        arrive(src, a_minus + 2 * r)
        send(src, src, dev(y, z, c, x + 1), a_far + 2 * r)
        src = abuf.at[r, :, :, lanes(1, x + 1)]
        arrive(src, a_plus + 2 * r + 1)
        send(src, src, dev(y, z, c, x + 3), a_far + 2 * r + 1)

    def finish_a(r):
        a_own[r].wait()
        arrive(abuf.at[r, :, :, lanes(oc, x)], a_part + r)
        arrive(abuf.at[r, :, :, lanes(1, x + 3)], a_minus + 2 * r + 1)
        arrive(abuf.at[r, :, :, lanes(0, x + 1)], a_plus + 2 * r)
        for group in range(2):
            arrive(abuf.at[r, :, :, lanes(group, x + 2)], a_far + 2 * r + group)

    def block_of(s, at=None):
        at = zlo if at is None else at
        pair = at // 2
        low = at % 2
        return (at, 2 * pair + 1 - low, 3 - at, 2 * (1 - pair) + low)[s]

    def half(h):
        return pl.ds(256 * h, 256)

    def send_c(h, s):
        dst = cbuf.at[zlo, c, :, :, half(h)]
        if s == 0:
            send(cot.at[:, zlo, :, half(h)], dst, partner, c_part + 4 * h)
        else:
            to = block_of(s)
            send(cot.at[:, to, :, half(h)], dst, dev(y, zhi * 4 + to, c, x), c_peer + 4 * h + s)

    def send_d():
        send(drift.at[:, oc], dbuf.at[1], partner, d_part)

    def pass_c(h, s):
        src = cbuf.at[block_of(s), c, :, :, half(h)]
        arrive(src, c_peer + 4 * h + s)
        send(src, src, partner, c_part + 4 * h + s)

    def finish_c(h, s):
        if h == 0 and s == 0:
            c_own.wait()
        arrive(cbuf.at[block_of(s), oc, :, :, half(h)], c_part + 4 * h + s)

    have = set()

    def once(step, *args):
        if (step, args) not in have:
            have.add((step, args))
            step(*args)

    def cut(n):
        return n % 4, half(n // 4)

    y_first = take("r", 32)
    y_all = take("r", 32)

    def finish_d():
        d_own.wait()
        arrive(dbuf.at[1], d_part)

    def compute(n, s):
        unit = n * 4 + s
        r, cols = cut(n)
        wide = 256
        q = block_of(s)
        once(finish_a, r)
        once(finish_c, n // 4, s)
        once(finish_d)
        lhs = abuf[r].reshape(512, 1024)
        rhs = cbuf[q, :, :, :, cols].reshape(1024, wide)
        total = jnp.dot(lhs, rhs, preferred_element_type=F32)
        if s == 0:
            total = total + dbuf[0, :, r, :, cols].reshape(512, wide).astype(F32)
            total = total + dbuf[1, :, r, :, cols].reshape(512, wide).astype(F32)
        pbuf[r, s, :, :, :, cols] = total.astype(BF16).reshape(4, 2, 64, wide)
        far, near, back = (y + 2) % 4, (y + 1) % 4, (y + 3) % 4
        send(pbuf.at[r, s, far, 0, :, cols], y1.at[0, r, s, :, cols], up, y_first + unit)
        send(pbuf.at[r, s, far, 1, :, cols], y1.at[1, r, s, :, cols], down, y_first + unit)
        send(pbuf.at[r, s, near, 1, :, cols], y2.at[0, r, s, 1, :, cols], up, y_all + unit)
        send(pbuf.at[r, s, back, 0, :, cols], y2.at[1, r, s, 0, :, cols], down, y_all + unit)

    def relay_y(n, s):
        unit = n * 4 + s
        r, cols = cut(n)
        arrive(y1.at[:, r, s, :, cols], y_first + unit)
        for way, yy in enumerate(((y + 1) % 4, (y + 3) % 4)):
            part = pbuf.at[r, s, yy, way, :, cols]
            came = y1.at[way, r, s, :, cols]
            part[...] = (part[...].astype(F32) + came[...].astype(F32)).astype(BF16)
            send(part, y2.at[way, r, s, way, :, cols], (up, down)[way], y_all + unit)

    def finish_y(n, s):
        unit = n * 4 + s
        r, cols = cut(n)
        q = block_of(s)
        arrive(y2.at[:, r, s, :, :, cols], y_all + unit)
        for hi in range(2):
            total = (pbuf[r, s, y, hi, :, cols].astype(F32) + y2[0, r, s, hi, :, cols].astype(F32)
                     + y2[1, r, s, hi, :, cols].astype(F32)).astype(BF16)
            for pz in range(4):
                rbuf[r, hi * 4 + pz, q, :, cols] = total[pz * 16:(pz + 1) * 16]

    z_in = take("r", 32)

    def skip_z(step):
        cols = half(1)
        every = pl.ds(0, 4)
        base = z_in + 28
        if step == 1:
            arrive(zr.at[0, 3, 0, :, :, cols], base)
            arrive(zr.at[:, 3, 1, :, :, cols], base + 1)
        elif step == 2:
            arrive(zr.at[:, 3, 2, :, :, cols], base + 2)
            arrive(zr.at[:, 3, 3, :, :, cols], base + 3)
            return
        for way in range(2):
            sign = 1 - 2 * way
            one, two = (z + 8 + sign) % 8, (z + 8 + 2 * sign) % 8
            some = pl.ds(2 * way, 2)
            first = zr.at[0, 3, 0, some, :, cols]
            second = zr.at[way, 3, 1, :, :, cols]

            def held(zz, part=every):
                return rbuf.at[3, zz % 8, part, :, cols]

            if step == 0:
                to = dev(y, two, c, x)
                send(held(z + 4, some), first, to, base)
                send(held(z + 8 + 3 * sign), second, to, base + 1)
                continue
            for i, (zz, part, came) in enumerate(((two, some, first), (one, every, second))):
                own = held(zz, part)
                own[...] = (own[...].astype(F32) + came[...].astype(F32)).astype(BF16)
                send(held(zz), zr.at[way, 3, 2 + i, :, :, cols], dev(y, zz, c, x), base + 2 + i)

    def ring_z(n, step):
        if n == 7:
            skip_z(step)
            return
        r, cols = cut(n)
        base = z_in + 4 * n + step
        if step == 1:
            arrive(zr.at[0, r, 0, :, :, cols], base - 1)
        elif step > 1:
            arrive(zr.at[:, r, step - 1, :, :, cols], base - 1)
        if step == 4:
            return
        for way in range(2):
            to = (zup, zdown)[way]
            some = pl.ds(2 * way, 2)
            if step == 0:
                send(rbuf.at[r, (z + 4) % 8, some, :, cols], zr.at[0, r, 0, some, :, cols], to, base)
                continue
            target = (z + (4 - step)) % 8 if way == 0 else (z + 4 + step) % 8
            if step == 1:
                came, own = zr.at[0, r, 0, some, :, cols], rbuf.at[r, target, some, :, cols]
            else:
                came, own = zr.at[way, r, step - 1, :, :, cols], rbuf.at[r, target, :, :, cols]
            own[...] = (own[...].astype(F32) + came[...].astype(F32)).astype(BF16)
            send(rbuf.at[r, target, :, :, cols], zr.at[way, r, step, :, :, cols], to, base)

    s_in = take("r", 4)

    def send_state():
        o_own.wait()
        m_own.wait()
        tloc[...] = obuf[...] - outer_rate * nesterov * nesterov * mbuf[...]
        for d in (1, 3, 2):
            xx = (x + d) % 4
            send(tloc.at[:, columns(xx)], tbuf.at[x], dev(y, z, c, xx), s_in + d)
        tbuf[x] = tloc[:, columns(x)]

    def finish_state():
        for d in (1, 3, 2):
            arrive(tbuf.at[(x - d) % 4], s_in + d)

    b_in = take("r", 2)
    r_two = take("r", 8)

    def update(n):
        r, cut_cols = cut(n)
        first, wide = 256 * (n // 4), 256
        once(finish_state)
        for q in range(4):
            cols = pl.ds(q * 512 + first, wide)
            total = rbuf[r, z, q, :, cut_cols].astype(F32)
            for way in range(2):
                for step in ((3,), (2, 3))[n == 7]:
                    total = total + zr[way, r, step, q, :, cut_cols].astype(F32)
            fbuf[r, q, :, cut_cols] = total.astype(BF16)
            average = fbuf[r, q, :, cut_cols].astype(F32) / 16
            weights = tbuf[r, :, cols] - outer_rate * (1 + nesterov) * average
            wbuf[r, q, :, cut_cols] = weights.astype(BF16)
        own = wout.at[y, zhi, c, r, zlo, :, cut_cols]
        for k in (4, 3, 5, 2, 6, 1, 7):
            zz = (z + k) % 8
            send(wbuf.at[r, zz % 4, :, cut_cols], own, dev(y, zz, c, x), r_two + n)
        pltpu.make_async_copy(wbuf.at[r, zlo, :, cut_cols], own, rs.at[r_two + n]).start()
        src, dst = fbuf.at[r, :, :, cut_cols], xr.at[x, :, :, cut_cols]
        back = remote(src, dst, dev(y, z, c, r), b_in + n // 4, POOL + n)
        keep = pltpu.make_async_copy(src, dst, rs.at[b_in + n // 4])

        @pl.when(x != r)
        def _():
            back.start()

        @pl.when(x == r)
        def _():
            keep.start()

        def finish_back():
            @pl.when(x != r)
            def _():
                back.wait_send()

        kept.append(finish_back)

    kept = []

    def finish_outer():
        for finish in kept:
            finish()
        for h in range(2):
            arrive(xr.at[:, :, :, half(h)], b_in + h)
        for xx in range(4):
            for q in range(4):
                cols = pl.ds((xx * 4 + q) * 512, 512)
                average = xr[xx, q].astype(F32) / 16
                momentum = nesterov * mbuf[:, cols] + average
                nm_out[:, cols] = momentum
                no_out[:, cols] = obuf[:, cols] - outer_rate * (average + nesterov * momentum)

    r_up = take("r", 8)
    r_down = take("r", 8)
    r_far = take("r", 8)
    r_part = take("r", 8)

    def both(n, yy, cc):
        r, cols = cut(n)
        return wout.at[yy, :, cc, r, :, :, cols]

    def one_of(n, yy, hi, cc):
        r, cols = cut(n)
        return wout.at[yy, hi, cc, r, :, :, cols]

    def gather_own(n):
        arrive(both(n, y, c), r_two + n)
        src = both(n, y, c)
        send(src, src, up, r_down + n)
        send(src, src, down, r_up + n)
        send(src, src, partner, r_part + n)

    def gather_near(n):
        for way, yy in enumerate(((y + 3) % 4, (y + 1) % 4)):
            src = both(n, yy, c)
            arrive(src, (r_down, r_up)[way] + n)
            nearer = one_of(n, yy, way, c)
            send(nearer, nearer, (up, down)[way], r_far + n)
            send(src, src, partner, r_part + n)

    def gather_far(n):
        src = both(n, (y + 2) % 4, c)
        arrive(src, r_far + n)
        send(src, src, partner, r_part + n)

    def gather_done(n):
        r, cols = cut(n)
        arrive(wout.at[:, :, oc, r, :, :, cols], r_part + n)

    plan = [
        (0.0, send_a, 0), (0.0, send_c, 0, 0), (0.0, send_c, 0, 1), (0.0, send_c, 0, 2),
        (0.0, send_d), (0.0, send_c, 1, 0), (7.5, forward_a, 0), (7.5, send_a, 1), (7.6, send_c, 0, 3),
        (12.4, send_c, 1, 1), (18.0, forward_a, 1), (18.0, send_a, 2), (18.1, send_c, 1, 2),
        (23.5, send_c, 1, 3), (28.8, forward_a, 2), (28.8, send_a, 3), (28.9, send_state), (40.0, forward_a, 3),
    ]
    for h in range(2):
        for s in range(1, 4):
            plan.append((COTS[h][s] - 1.5, pass_c, h, s))
    ended = [0.0] * 8
    for n, s, ready, begun in reduction_order():
        plan.append((max(ready, begun - 3.0), compute, n, s))
        plan.append((begun + 4.2, relay_y, n, s))
        plan.append((begun + 8.4, finish_y, n, s))
        ended[n] = max(ended[n], begun + 8.5)
    ring = 45.0
    for n in range(8):
        ring = max(ended[n] + 0.8, ring + 4.0)
        pace, steps = (4.2, 4) if n < 7 else (5.5, 2)
        for step in range(steps + 1):
            plan.append((ring + pace * step, ring_z, n, step))
        stop = ring + pace * steps + 0.1
        begin = max(stop + 4.8, 84.0 + 1.5 * n)
        for when, step in ((stop, update), (begin, gather_own), (begin + 4.4, gather_near),
                           (begin + 8.2, gather_far), (150.0, gather_done)):
            plan.append((when, step, n))
    plan.append((149.0, finish_outer))
    plan.sort(key=lambda entry: entry[0])
    for _, step, *args in plan:
        step(*args)

    for finish in sends:
        finish()


def on_device(activations, cotangent, drift, outer_weights, momentum):
    cot = cotangent[0].reshape(4, 4, 128, 512)
    dr = drift[0].reshape(8, 2, 4, 64, 512)
    any_spec = pl.BlockSpec(memory_space=pl.ANY)
    vmem_spec = pl.BlockSpec(memory_space=pltpu.VMEM)
    hbm_spec = pl.BlockSpec(memory_space=pltpu.HBM)
    weights, new_outer, new_momentum = pl.pallas_call(
        kernel,
        out_shape=(
            pltpu.VMEM((4, 2, 2, 4, 4, 16, 512), BF16),
            pltpu.VMEM((16, 8192), F32),
            pltpu.VMEM((16, 8192), F32),
        ),
        in_specs=[hbm_spec] * 5,
        out_specs=[any_spec, vmem_spec, vmem_spec],
        scratch_shapes=[
            pltpu.VMEM((128, 4096), BF16),
            pltpu.VMEM((8, 2, 4, 64, 128), BF16),
            pltpu.VMEM((4, 8, 64, 1024), BF16),
            pltpu.VMEM((4, 2, 4, 128, 512), BF16),
            pltpu.VMEM((2, 8, 4, 64, 512), BF16),
            pltpu.VMEM((4, 4, 4, 2, 64, 512), BF16),
            pltpu.VMEM((2, 4, 4, 64, 512), BF16),
            pltpu.VMEM((2, 4, 4, 2, 64, 512), BF16),
            pltpu.VMEM((4, 8, 4, 16, 512), BF16),
            pltpu.VMEM((2, 4, 4, 4, 16, 512), BF16),
            pltpu.VMEM((4, 4, 16, 512), BF16),
            pltpu.VMEM((16, 8192), F32),
            pltpu.VMEM((16, 8192), F32),
            pltpu.VMEM((16, 8192), F32),
            pltpu.VMEM((4, 16, 2048), F32),
            pltpu.VMEM((4, 4, 16, 512), BF16),
            pltpu.VMEM((4, 4, 16, 512), BF16),
            pltpu.SemaphoreType.DMA((POOL + 8,)),
            pltpu.SemaphoreType.DMA((N_RECV,)),
            pltpu.SemaphoreType.DMA((N_LOCAL,)),
        ],
        compiler_params=pltpu.CompilerParams(
            collective_id=0, has_side_effects=True, vmem_limit_bytes=54 * 1024 * 1024
        ),
        name="outer_step",
    )(activations[0], cot, dr, outer_weights, momentum)
    return weights.reshape(4096, 512), new_outer, new_momentum


def solution(mesh):
    in_specs = (
        P("rep", "tp", None),
        P("rep", None, "tp"),
        P("rep", None, "tp"),
        P(("rep", "tp"), None),
        P(("rep", "tp"), None),
    )
    out_specs = (P(None, "tp"), P(("rep", "tp"), None), P(("rep", "tp"), None))
    return jax.shard_map(
        on_device, mesh=mesh, in_specs=in_specs, out_specs=out_specs, check_vma=False
    )
```

```python
import functools

import jax
import jax.numpy as jnp
from jax import lax
from jax.experimental import pallas as pl
from jax.experimental.pallas import tpu as pltpu
from jax.sharding import PartitionSpec as P

outer_rate = 0.7
nesterov = 0.9

F32 = jnp.float32
BF16 = jnp.bfloat16
MESH = pl.DeviceIdType.MESH
POOL = 72
N_RECV = 192
N_LOCAL = 16

ACTS = (12.5, 23.5, 35.0, 47.0)
COTS = ((1.0, 13.0, 16.0, 28.0), (1.0, 24.0, 41.0, 50.0))
PACE = 2.08


def reduction_order():
    waiting = [(h * 4 + r, s, max(ACTS[r], COTS[h][s]))
               for h in range(2) for r in range(4) for s in range(4)]
    now, order = 0.0, []
    while waiting:
        now = max(now, min(ready for _, _, ready in waiting))
        unit = next(u for u in waiting if u[2] <= now)
        waiting.remove(unit)
        order.append((unit[0], unit[1], unit[2], now))
        now += PACE
    return order


def kernel(act, cot, drift, outer, mom, wout, no_out, nm_out,
           av, atv, abuf, cbuf, dbuf, pbuf, y1, y2, rbuf, zr, wbuf, obuf, mbuf, tloc, tbuf, fbuf, xr,
           ss, rs, ls):
    rep = lax.axis_index("rep")
    tp = lax.axis_index("tp")
    y = rep // 4
    zhi = (rep // 2) % 2
    c = rep % 2
    x = tp // 4
    zlo = tp % 4
    z = zhi * 4 + zlo
    oc = 1 - c

    def dev(yy, zz, cc, xx):
        return ((yy % 4) * 4 + ((zz % 8) // 4) * 2 + cc, (xx % 4) * 4 + (zz % 4))

    counts = {"s": 0, "r": 0, "l": 0}
    sends = []

    def take(kind, n=1):
        base = counts[kind]
        counts[kind] += n
        return base

    def remote(src, dst, to, rsem, ssem):
        return pltpu.make_async_remote_copy(
            src_ref=src, dst_ref=dst, send_sem=ss.at[ssem], recv_sem=rs.at[rsem],
            device_id=to, device_id_type=MESH)

    def send(src, dst, to, rsem):
        if len(sends) == POOL:
            sends.pop(0)()
        copy = remote(src, dst, to, rsem, take("s") % POOL)
        copy.start()
        sends.append(copy.wait_send)

    def arrive(ref, rsem):
        pltpu.make_async_copy(ref, ref, rs.at[rsem]).wait()

    def local(src, dst):
        copy = pltpu.make_async_copy(src, dst, ls.at[take("l")])
        copy.start()
        return copy

    partner = dev(y, z, oc, x)
    up, down = dev(y + 1, z, c, x), dev(y - 1, z, c, x)
    zup, zdown = dev(y, z + 1, c, x), dev(y, z - 1, c, x)

    greeted = [dev(y, z + k, c, x) for k in (4, 3, 5, 2, 6, 1, 7)]
    greeted += [dev(y, z, c, x + 2)]
    greeted += [dev(y, z, cc, x + d) for d in (1, 3) for cc in (0, 1)]
    greeted += [up, down, partner]
    barrier = pltpu.get_barrier_semaphore()
    for other in greeted:
        pl.semaphore_signal(barrier, inc=1, device_id=other, device_id_type=MESH)

    def lanes(group, xx):
        return pl.ds(pl.multiple_of((group * 4 + xx % 4) * 128, 128), 128)

    def columns(xx):
        return pl.ds(pl.multiple_of((xx % 4) * 2048, 2048), 2048)

    a_in = local(act, av)
    c_own = local(cot.at[:, zlo], cbuf.at[zlo, c])
    d_own = local(drift.at[:, c], dbuf.at[0])
    o_own = local(outer, obuf)
    m_own = local(mom, mbuf)
    a_in.wait()
    for j in range(32):
        tile = av[:, pl.ds(j * 128, 128)].T
        for i in range(2):
            atv[j // 4, (j // 2) % 2, 2 * (j % 2) + i] = tile[i * 64:(i + 1) * 64]
    pl.semaphore_wait(barrier, len(greeted))

    a_part = take("r", 4)
    a_minus = take("r", 8)
    a_plus = take("r", 8)
    a_far = take("r", 8)
    c_part = take("r", 8)
    c_peer = take("r", 8)
    d_part = take("r", 1)
    a_own = []

    def send_a(r):
        dst = abuf.at[r, :, :, lanes(c, x)]
        for turn in range(2):
            ahead = 1 - 2 * c if turn == 0 else 2 * c - 1
            rsem = a_minus + 2 * r + c + 8 * (c if turn == 0 else oc)
            send(atv.at[:, c, r], dst, dev(y, z, c, x + 4 + ahead), rsem)
            send(atv.at[:, oc, r], dst, dev(y, z, oc, x + 4 + ahead), rsem)
        send(atv.at[:, oc, r], dst, partner, a_part + r)
        a_own.append(local(atv.at[:, c, r], dst))

    def forward_a(r):
        src = abuf.at[r, :, :, lanes(0, x + 3)]
        arrive(src, a_minus + 2 * r)
        send(src, src, dev(y, z, c, x + 1), a_far + 2 * r)
        src = abuf.at[r, :, :, lanes(1, x + 1)]
        arrive(src, a_plus + 2 * r + 1)
        send(src, src, dev(y, z, c, x + 3), a_far + 2 * r + 1)

    def finish_a(r):
        a_own[r].wait()
        arrive(abuf.at[r, :, :, lanes(oc, x)], a_part + r)
        arrive(abuf.at[r, :, :, lanes(1, x + 3)], a_minus + 2 * r + 1)
        arrive(abuf.at[r, :, :, lanes(0, x + 1)], a_plus + 2 * r)
        for group in range(2):
            arrive(abuf.at[r, :, :, lanes(group, x + 2)], a_far + 2 * r + group)

    def block_of(s, at=None):
        at = zlo if at is None else at
        pair = at // 2
        low = at % 2
        return (at, 2 * pair + 1 - low, 3 - at, 2 * (1 - pair) + low)[s]

    def half(h):
        return pl.ds(256 * h, 256)

    def send_c(h, s):
        dst = cbuf.at[zlo, c, :, :, half(h)]
        if s == 0:
            send(cot.at[:, zlo, :, half(h)], dst, partner, c_part + 4 * h)
        else:
            to = block_of(s)
            send(cot.at[:, to, :, half(h)], dst, dev(y, zhi * 4 + to, c, x), c_peer + 4 * h + s)

    def send_d():
        send(drift.at[:, oc], dbuf.at[1], partner, d_part)

    def pass_c(h, s):
        src = cbuf.at[block_of(s), c, :, :, half(h)]
        arrive(src, c_peer + 4 * h + s)
        send(src, src, partner, c_part + 4 * h + s)

    def finish_c(h, s):
        if h == 0 and s == 0:
            c_own.wait()
        arrive(cbuf.at[block_of(s), oc, :, :, half(h)], c_part + 4 * h + s)

    have = set()

    def once(step, *args):
        if (step, args) not in have:
            have.add((step, args))
            step(*args)

    def cut(n):
        return n % 4, half(n // 4)

    y_first = take("r", 32)
    y_all = take("r", 32)

    def finish_d():
        d_own.wait()
        arrive(dbuf.at[1], d_part)

    def compute(n, s):
        unit = n * 4 + s
        r, cols = cut(n)
        wide = 256
        q = block_of(s)
        once(finish_a, r)
        once(finish_c, n // 4, s)
        once(finish_d)
        lhs = abuf[r].reshape(512, 1024)
        rhs = cbuf[q, :, :, :, cols].reshape(1024, wide)
        total = jnp.dot(lhs, rhs, preferred_element_type=F32)
        if s == 0:
            total = total + dbuf[0, :, r, :, cols].reshape(512, wide).astype(F32)
            total = total + dbuf[1, :, r, :, cols].reshape(512, wide).astype(F32)
        pbuf[r, s, :, :, :, cols] = total.astype(BF16).reshape(4, 2, 64, wide)
        far, near, back = (y + 2) % 4, (y + 1) % 4, (y + 3) % 4
        send(pbuf.at[r, s, far, 0, :, cols], y1.at[0, r, s, :, cols], up, y_first + unit)
        send(pbuf.at[r, s, far, 1, :, cols], y1.at[1, r, s, :, cols], down, y_first + unit)
        send(pbuf.at[r, s, near, 1, :, cols], y2.at[0, r, s, 1, :, cols], up, y_all + unit)
        send(pbuf.at[r, s, back, 0, :, cols], y2.at[1, r, s, 0, :, cols], down, y_all + unit)

    def relay_y(n, s):
        unit = n * 4 + s
        r, cols = cut(n)
        arrive(y1.at[:, r, s, :, cols], y_first + unit)
        for way, yy in enumerate(((y + 1) % 4, (y + 3) % 4)):
            part = pbuf.at[r, s, yy, way, :, cols]
            came = y1.at[way, r, s, :, cols]
            part[...] = (part[...].astype(F32) + came[...].astype(F32)).astype(BF16)
            send(part, y2.at[way, r, s, way, :, cols], (up, down)[way], y_all + unit)

    def finish_y(n, s):
        unit = n * 4 + s
        r, cols = cut(n)
        q = block_of(s)
        arrive(y2.at[:, r, s, :, :, cols], y_all + unit)
        for hi in range(2):
            total = (pbuf[r, s, y, hi, :, cols].astype(F32) + y2[0, r, s, hi, :, cols].astype(F32)
                     + y2[1, r, s, hi, :, cols].astype(F32)).astype(BF16)
            for pz in range(4):
                rbuf[r, hi * 4 + pz, q, :, cols] = total[pz * 16:(pz + 1) * 16]

    z_in = take("r", 32)

    def skip_z(step):
        cols = half(1)
        every = pl.ds(0, 4)
        base = z_in + 28
        if step == 1:
            arrive(zr.at[0, 3, 0, :, :, cols], base)
            arrive(zr.at[:, 3, 1, :, :, cols], base + 1)
        elif step == 2:
            arrive(zr.at[:, 3, 2, :, :, cols], base + 2)
            arrive(zr.at[:, 3, 3, :, :, cols], base + 3)
            return
        for way in range(2):
            sign = 1 - 2 * way
            one, two = (z + 8 + sign) % 8, (z + 8 + 2 * sign) % 8
            some = pl.ds(2 * way, 2)
            first = zr.at[0, 3, 0, some, :, cols]
            second = zr.at[way, 3, 1, :, :, cols]

            def held(zz, part=every):
                return rbuf.at[3, zz % 8, part, :, cols]

            if step == 0:
                to = dev(y, two, c, x)
                send(held(z + 4, some), first, to, base)
                send(held(z + 8 + 3 * sign), second, to, base + 1)
                continue
            for i, (zz, part, came) in enumerate(((two, some, first), (one, every, second))):
                own = held(zz, part)
                own[...] = (own[...].astype(F32) + came[...].astype(F32)).astype(BF16)
                send(held(zz), zr.at[way, 3, 2 + i, :, :, cols], dev(y, zz, c, x), base + 2 + i)

    def ring_z(n, step):
        if n == 7:
            skip_z(step)
            return
        r, cols = cut(n)
        base = z_in + 4 * n + step
        if step == 1:
            arrive(zr.at[0, r, 0, :, :, cols], base - 1)
        elif step > 1:
            arrive(zr.at[:, r, step - 1, :, :, cols], base - 1)
        if step == 4:
            return
        for way in range(2):
            to = (zup, zdown)[way]
            some = pl.ds(2 * way, 2)
            if step == 0:
                send(rbuf.at[r, (z + 4) % 8, some, :, cols], zr.at[0, r, 0, some, :, cols], to, base)
                continue
            target = (z + (4 - step)) % 8 if way == 0 else (z + 4 + step) % 8
            if step == 1:
                came, own = zr.at[0, r, 0, some, :, cols], rbuf.at[r, target, some, :, cols]
            else:
                came, own = zr.at[way, r, step - 1, :, :, cols], rbuf.at[r, target, :, :, cols]
            own[...] = (own[...].astype(F32) + came[...].astype(F32)).astype(BF16)
            send(rbuf.at[r, target, :, :, cols], zr.at[way, r, step, :, :, cols], to, base)

    s_in = take("r", 4)

    def send_state():
        o_own.wait()
        m_own.wait()
        tloc[...] = obuf[...] - outer_rate * nesterov * nesterov * mbuf[...]
        for d in (1, 3, 2):
            xx = (x + d) % 4
            send(tloc.at[:, columns(xx)], tbuf.at[x], dev(y, z, c, xx), s_in + d)
        tbuf[x] = tloc[:, columns(x)]

    def finish_state():
        for d in (1, 3, 2):
            arrive(tbuf.at[(x - d) % 4], s_in + d)

    b_in = take("r", 2)
    r_two = take("r", 8)

    def update(n):
        r, cut_cols = cut(n)
        first, wide = 256 * (n // 4), 256
        once(finish_state)
        for q in range(4):
            cols = pl.ds(q * 512 + first, wide)
            total = rbuf[r, z, q, :, cut_cols].astype(F32)
            for way in range(2):
                for step in ((3,), (2, 3))[n == 7]:
                    total = total + zr[way, r, step, q, :, cut_cols].astype(F32)
            fbuf[r, q, :, cut_cols] = total.astype(BF16)
            average = fbuf[r, q, :, cut_cols].astype(F32) / 16
            weights = tbuf[r, :, cols] - outer_rate * (1 + nesterov) * average
            wbuf[r, q, :, cut_cols] = weights.astype(BF16)
        own = wout.at[y, zhi, c, r, zlo, :, cut_cols]
        for k in (4, 3, 5, 2, 6, 1, 7):
            zz = (z + k) % 8
            send(wbuf.at[r, zz % 4, :, cut_cols], own, dev(y, zz, c, x), r_two + n)
        pltpu.make_async_copy(wbuf.at[r, zlo, :, cut_cols], own, rs.at[r_two + n]).start()
        src, dst = fbuf.at[r, :, :, cut_cols], xr.at[x, :, :, cut_cols]
        back = remote(src, dst, dev(y, z, c, r), b_in + n // 4, POOL + n)
        keep = pltpu.make_async_copy(src, dst, rs.at[b_in + n // 4])

        @pl.when(x != r)
        def _():
            back.start()

        @pl.when(x == r)
        def _():
            keep.start()

        def finish_back():
            @pl.when(x != r)
            def _():
                back.wait_send()

        kept.append(finish_back)

    kept = []

    def finish_outer():
        for finish in kept:
            finish()
        for h in range(2):
            arrive(xr.at[:, :, :, half(h)], b_in + h)
        for xx in range(4):
            for q in range(4):
                cols = pl.ds((xx * 4 + q) * 512, 512)
                average = xr[xx, q].astype(F32) / 16
                momentum = nesterov * mbuf[:, cols] + average
                nm_out[:, cols] = momentum
                no_out[:, cols] = obuf[:, cols] - outer_rate * (average + nesterov * momentum)

    r_up = take("r", 8)
    r_down = take("r", 8)
    r_far = take("r", 8)
    r_part = take("r", 8)

    def both(n, yy, cc):
        r, cols = cut(n)
        return wout.at[yy, :, cc, r, :, :, cols]

    def one_of(n, yy, hi, cc):
        r, cols = cut(n)
        return wout.at[yy, hi, cc, r, :, :, cols]

    def gather_own(n):
        arrive(both(n, y, c), r_two + n)
        src = both(n, y, c)
        send(src, src, up, r_down + n)
        send(src, src, down, r_up + n)
        send(src, src, partner, r_part + n)

    def gather_near(n):
        for way, yy in enumerate(((y + 3) % 4, (y + 1) % 4)):
            src = both(n, yy, c)
            arrive(src, (r_down, r_up)[way] + n)
            nearer = one_of(n, yy, way, c)
            send(nearer, nearer, (up, down)[way], r_far + n)
            send(src, src, partner, r_part + n)

    def gather_far(n):
        src = both(n, (y + 2) % 4, c)
        arrive(src, r_far + n)
        send(src, src, partner, r_part + n)

    def gather_done(n):
        r, cols = cut(n)
        arrive(wout.at[:, :, oc, r, :, :, cols], r_part + n)

    plan = [
        (0.0, send_a, 0), (0.0, send_c, 0, 0), (0.0, send_c, 0, 1), (0.0, send_c, 0, 2),
        (0.0, send_d), (0.0, send_c, 1, 0), (7.5, forward_a, 0), (7.5, send_a, 1), (7.6, send_c, 0, 3),
        (12.4, send_c, 1, 1), (18.0, forward_a, 1), (18.0, send_a, 2), (18.1, send_c, 1, 2),
        (23.5, send_c, 1, 3), (28.8, forward_a, 2), (28.8, send_a, 3), (28.9, send_state), (40.0, forward_a, 3),
    ]
    for h in range(2):
        for s in range(1, 4):
            plan.append((COTS[h][s] - 1.5, pass_c, h, s))
    ended = [0.0] * 8
    for n, s, ready, begun in reduction_order():
        plan.append((max(ready, begun - 3.0), compute, n, s))
        plan.append((begun + 4.2, relay_y, n, s))
        plan.append((begun + 8.4, finish_y, n, s))
        ended[n] = max(ended[n], begun + 8.5)
    ring = 45.0
    for n in range(8):
        ring = max(ended[n] + 0.8, ring + 4.0)
        pace, steps = (4.2, 4) if n < 7 else (5.5, 2)
        for step in range(steps + 1):
            plan.append((ring + pace * step, ring_z, n, step))
        stop = ring + pace * steps + 0.1
        begin = max(stop + 4.8, 87.5 + 1.5 * n)
        for when, step in ((stop, update), (begin, gather_own), (begin + 4.4, gather_near),
                           (begin + 8.2, gather_far), (150.0, gather_done)):
            plan.append((when, step, n))
    plan.append((149.0, finish_outer))
    plan.sort(key=lambda entry: entry[0])
    for _, step, *args in plan:
        step(*args)

    for finish in sends:
        finish()


def on_device(activations, cotangent, drift, outer_weights, momentum):
    cot = cotangent[0].reshape(4, 4, 128, 512)
    dr = drift[0].reshape(8, 2, 4, 64, 512)
    any_spec = pl.BlockSpec(memory_space=pl.ANY)
    vmem_spec = pl.BlockSpec(memory_space=pltpu.VMEM)
    hbm_spec = pl.BlockSpec(memory_space=pltpu.HBM)
    weights, new_outer, new_momentum = pl.pallas_call(
        kernel,
        out_shape=(
            pltpu.VMEM((4, 2, 2, 4, 4, 16, 512), BF16),
            pltpu.VMEM((16, 8192), F32),
            pltpu.VMEM((16, 8192), F32),
        ),
        in_specs=[hbm_spec] * 5,
        out_specs=[any_spec, vmem_spec, vmem_spec],
        scratch_shapes=[
            pltpu.VMEM((128, 4096), BF16),
            pltpu.VMEM((8, 2, 4, 64, 128), BF16),
            pltpu.VMEM((4, 8, 64, 1024), BF16),
            pltpu.VMEM((4, 2, 4, 128, 512), BF16),
            pltpu.VMEM((2, 8, 4, 64, 512), BF16),
            pltpu.VMEM((4, 4, 4, 2, 64, 512), BF16),
            pltpu.VMEM((2, 4, 4, 64, 512), BF16),
            pltpu.VMEM((2, 4, 4, 2, 64, 512), BF16),
            pltpu.VMEM((4, 8, 4, 16, 512), BF16),
            pltpu.VMEM((2, 4, 4, 4, 16, 512), BF16),
            pltpu.VMEM((4, 4, 16, 512), BF16),
            pltpu.VMEM((16, 8192), F32),
            pltpu.VMEM((16, 8192), F32),
            pltpu.VMEM((16, 8192), F32),
            pltpu.VMEM((4, 16, 2048), F32),
            pltpu.VMEM((4, 4, 16, 512), BF16),
            pltpu.VMEM((4, 4, 16, 512), BF16),
            pltpu.SemaphoreType.DMA((POOL + 8,)),
            pltpu.SemaphoreType.DMA((N_RECV,)),
            pltpu.SemaphoreType.DMA((N_LOCAL,)),
        ],
        compiler_params=pltpu.CompilerParams(
            collective_id=0, has_side_effects=True, vmem_limit_bytes=54 * 1024 * 1024
        ),
        name="outer_step",
    )(activations[0], cot, dr, outer_weights, momentum)
    return weights.reshape(4096, 512), new_outer, new_momentum


def solution(mesh):
    in_specs = (
        P("rep", "tp", None),
        P("rep", None, "tp"),
        P("rep", None, "tp"),
        P(("rep", "tp"), None),
        P(("rep", "tp"), None),
    )
    out_specs = (P(None, "tp"), P(("rep", "tp"), None), P(("rep", "tp"), None))
    return jax.shard_map(
        on_device, mesh=mesh, in_specs=in_specs, out_specs=out_specs, check_vma=False
    )
```
